256 devices in a mesh: groups: 2 (over z), ref: 128 (over x, y, core).
Axes of the slice: x: 8, y: 8, z: 2, core: 2. Of those that a mesh axis runs over, the one named last changes fastest.
The devices are a block of a 8x8x16 slice.
Arguments:
- long_series: bfloat16 [1048576], P(('groups', 'ref')), parts along dimension 0, may hold values from -12 to 12
- queries: bfloat16 [512, 1024], P(('groups', 'ref')), parts along dimension 0, may hold values from -48 to 48
- lengths: int32 [512], P(('groups', 'ref')), parts along dimension 0, may hold values from 512 to 1024, as said below
- groups: int32 [512], P(('groups', 'ref')), parts along dimension 0, may hold values from 0 to 127, as said below
Outputs:
- profile: float32 [512, 1024], P(('groups', 'ref')), parts along dimension 0
The draws below stay inside these ranges and needn't reach their ends.
There are 2 independent parts, one for each index of `groups`. The reference program is written for one: setup_inputs(seed, part) draws one part's arguments, and reference() takes and returns one part's arrays. A program takes and returns all parts, laid end to end along the dimension named above; each array names one. Nothing has to cross between parts.
Inputs may be any that keep to these rules, and one draw needn't show every extreme that they name: `lengths`: multiples of 128. `groups`: region g holds reference blocks g * 1 to (g + 1) * 1 - 1; at most 4 queries name one region, and one region is named by exactly 4.
All inputs are finite; a program needn't handle non-finite values.
Results may differ from the reference program's by a relative error of at most 0.0003.
Values may be sent and summed in bfloat16 or wider, within the bound.
No kernel may reach another device: no remote copies, remote signals or barrier semaphores. Data moves between devices by JAX's collectives and lax.ppermute only.
A program may use at most 64 MiB of HBM per device.

```python
import math
import jax
import jax.numpy as jnp
from jax import lax

M = 256
LQ = 1024
RDEV = 4096
GDEV = 1
RMAX = 4
NQ = 256
NR = 524288
NGRP = 128


def make_join(key):
    blocks = NR // 128
    values = jax.random.normal(jax.random.fold_in(key, 1), (NR,), jnp.float32)
    shifts = 0.5 * jax.random.normal(jax.random.fold_in(key, 2), (blocks,), jnp.float32)
    scales = jnp.exp(jax.random.uniform(jax.random.fold_in(key, 3), (blocks,), jnp.float32, math.log(0.5), math.log(2.0)))
    series = jnp.clip(values * jnp.repeat(scales, 128) + jnp.repeat(shifts, 128), -12.0, 12.0)
    order = jax.random.permutation(jax.random.fold_in(key, 4), NQ)
    position = jnp.argsort(order)
    leader = jax.random.randint(jax.random.fold_in(key, 5), (), 0, NGRP)
    others = (leader + 1 + (position - RMAX) % (NGRP - 1)) % NGRP
    groups = jnp.where(position < RMAX, leader, others).astype(jnp.int32)
    copies = LQ // M
    starts = groups[:, None] * (GDEV * RDEV) + jax.random.randint(jax.random.fold_in(key, 6), (NQ, copies), 0, GDEV * RDEV - M + 1)
    gather_index = (starts[:, :, None] + jnp.arange(M, dtype=jnp.int32)[None, None, :]).reshape(NQ, LQ)
    copied = series[gather_index]
    noise_level = jnp.exp(jax.random.uniform(jax.random.fold_in(key, 7), (NQ, LQ // 128), jnp.float32, math.log(0.05), math.log(3.0)))
    noise = jax.random.normal(jax.random.fold_in(key, 8), (NQ, LQ), jnp.float32)
    made = copied + jnp.repeat(noise_level, 128, axis=1) * noise
    return (series, jnp.clip(made, -48.0, 48.0), groups)


def draw_long_series(key, part):
    return make_join(key)[0].astype(jnp.bfloat16)


def draw_queries(key, part):
    return make_join(key)[1].astype(jnp.bfloat16)


def draw_groups(key, part):
    return make_join(key)[2]


def draw_lengths(key, part):
    units = jax.random.randint(jax.random.fold_in(key, 31), (NQ,), LQ // 256, LQ // 128 + 1)
    sized = 128 * units
    return sized.at[0].set(LQ).at[1].set(LQ // 2).astype(jnp.int32)


def setup_inputs(seed: int = 0, part: int = 0) -> dict:
    keys = jax.random.split(jax.random.key(seed), 5)
    own_keys = jax.random.split(jax.random.fold_in(keys[4], part), 5)
    long_series = draw_long_series(jax.random.fold_in(jax.random.fold_in(keys[4], part), 71), part)
    queries = draw_queries(jax.random.fold_in(jax.random.fold_in(keys[4], part), 71), part)
    lengths = draw_lengths(jax.random.fold_in(jax.random.fold_in(keys[4], part), 71), part)
    groups = draw_groups(jax.random.fold_in(jax.random.fold_in(keys[4], part), 71), part)
    return dict(long_series=long_series, queries=queries, lengths=lengths, groups=groups)


SPREAD_FLOOR = 0.25

def window_stats(series, count):
    offsets_grid = jnp.arange(count, dtype=jnp.int32)[:, None] + jnp.arange(M, dtype=jnp.int32)[None, :]
    windows = series[offsets_grid]
    values = windows.astype(jnp.float32)
    centre = lax.optimization_barrier(jnp.mean(values, axis=1))
    spread = jnp.sqrt(lax.optimization_barrier(jnp.mean((values - centre[:, None]) ** 2, axis=1)) + SPREAD_FLOOR)
    return (windows, centre, spread)

def best_match(query_set, ref_set, usable):
    query_windows, query_centre, query_spread = query_set
    ref_windows, ref_centre, ref_spread = ref_set
    products = lax.dot_general(query_windows.astype(jnp.float32), ref_windows.astype(jnp.float32), (((1,), (1,)), ((), ())), precision=lax.Precision.HIGHEST, preferred_element_type=jnp.float32)
    correlation = (products - M * query_centre[:, None] * ref_centre[None, :]) / (M * query_spread[:, None] * ref_spread[None, :])
    correlation = jnp.where(usable[None, :], correlation, -2.0)
    return lax.optimization_barrier(jnp.max(correlation, axis=1))

def reference(long_series, queries, lengths, groups):
    overall = long_series.shape[0]
    padded = jnp.concatenate([long_series, jnp.zeros((M,), jnp.bfloat16)])

    def match_query(entry_pair):
        series, region = entry_pair
        query_set = window_stats(jnp.concatenate([series, jnp.zeros((M,), jnp.bfloat16)]), LQ)
        best_so_far = jnp.full((LQ,), -2.0, jnp.float32)
        for offset in range(GDEV):
            block_index = region * GDEV + offset
            first_cell = (block_index * RDEV).astype(jnp.int32)
            segment = lax.dynamic_slice_in_dim(padded, first_cell, RDEV + M)
            ref_set = window_stats(segment, RDEV)
            usable = first_cell + jnp.arange(RDEV, dtype=jnp.int32) <= overall - M
            best_so_far = jnp.maximum(best_so_far, best_match(query_set, ref_set, usable))
        return best_so_far
    best_values = lax.map(match_query, (queries, groups))
    live_points = jnp.arange(LQ, dtype=jnp.int32)[None, :] <= lengths[:, None] - M
    return jnp.where(live_points, 2.0 * (1.0 - best_values), 0.0)
```

```python
import functools
import math

import jax
import jax.numpy as jnp
from jax import lax
from jax.experimental import pallas as pl
from jax.experimental.pallas import tpu as pltpu
from jax.sharding import Mesh
from jax.sharding import PartitionSpec as P


M = 256
LANES = 128
SPREAD_FLOOR = 0.25
CORES = 2
NEVER = -3.0e38


def lane_iota(rows):
    return lax.broadcasted_iota(jnp.int32, (rows, LANES), 1)


def ahead(x, n, width):
    rows = x.shape[0]
    below = pltpu.roll(x, rows - 1, axis=0)
    if n == width:
        return below
    lane = lane_iota(rows)
    return jnp.where(lane < width - n, pltpu.roll(x, width - n, axis=1), pltpu.roll(below, width - n, axis=1))


def window_stats(x):
    total = x
    squares = jnp.zeros_like(x)
    n = 1
    while n < M:
        other = ahead(total, n, LANES)
        apart = total - other
        squares = squares + apart * apart * (0.5 / n)
        if n > 1:
            squares = squares + ahead(merged, n, LANES)
        merged = squares
        total = total + other
        n *= 2
    centre = total * (1.0 / M)
    spread = jnp.sqrt(squares * (1.0 / M) + SPREAD_FLOOR)
    return centre, spread


def hankel_rows(rows_of, blocks, put):
    sub = lax.broadcasted_iota(jnp.int32, (8, LANES), 0)
    lane = lane_iota(8)

    def rolled(b):
        base = jnp.broadcast_to(rows_of(b), (8, LANES))
        for bit in (1, 2, 4):
            base = jnp.where((sub & bit) != 0, pltpu.roll(base, LANES - bit, axis=1), base)
        return [base] + [pltpu.roll(base, LANES - 8 * t, axis=1) for t in range(1, LANES // 8)]

    own = rolled(0)
    for b in range(blocks):
        after = rolled(b + 1)
        pieces = [
            jnp.where(lane + sub < LANES - 8 * t, own[t], after[t]) for t in range(LANES // 8)
        ]
        put(b, jnp.concatenate(pieces, axis=0).astype(jnp.bfloat16))
        own = after


def prepare_queries(queries_ref, windows_ref, centre_ref, scale_ref):
    count, length = queries_ref.shape
    rows = length // LANES
    zero = jnp.zeros((1, LANES), jnp.float32)
    for s in range(count):
        parts = [
            queries_ref[s : s + 1, LANES * b : LANES * (b + 1)].astype(jnp.float32)
            for b in range(rows)
        ]

        def put(b, tile, s=s):
            windows_ref[s, LANES * b : LANES * (b + 1), :] = tile

        hankel_rows(lambda b: parts[b] if b < rows else zero, rows + 1, put)
        series = jnp.concatenate(parts + [zero] * 8, axis=0)
        centre, spread = window_stats(series)
        scale_ref[s] = 1.0 / (M * spread[:rows])
        for b in range(rows):
            wide = jnp.broadcast_to(centre[b : b + 1], (LANES, LANES))
            centre_ref[s, LANES * b : LANES * (b + 1), :] = wide.T


def answer(position_ref, *refs):
    *requests, blocks_ref, replies_ref = refs
    held, rows, _ = blocks_ref.shape
    peers, slots = len(requests), requests[0].shape[0]
    for distance, request in enumerate(requests):
        p = lax.rem(position_ref[0] + peers - distance, peers)
        for s in range(slots):
            want = lax.rem(request[s], held)
            follow = jnp.minimum(want + 1, held - 1)
            replies_ref[p, rows * s : rows * (s + 1), :] = blocks_ref[want]
            replies_ref[p, rows * slots + 8 * s : rows * slots + 8 * (s + 1), :] = blocks_ref[follow, 0:8, :]
        replies_ref[p, rows * slots + 8 * slots : rows * slots + 8 * slots + 8, :] = blocks_ref[0, 0:8, :]


def join(held, overall, groups_ref, lengths_ref, replies_ref, windows_ref, centre_ref, scale_ref, out_ref, ref_windows, weights, running):
    peers = replies_ref.shape[0]
    slots = groups_ref.shape[0]
    rows = (replies_ref.shape[1] - 8 * slots - 8) // slots
    block_len = rows * LANES
    query_len = centre_ref.shape[1]
    chunk = min(256, query_len)
    for s in range(slots):
        region = groups_ref[s]
        column = region // held
        place = lax.rem(region, held)
        block = replies_ref[column, rows * s : rows * (s + 1), :].astype(jnp.float32)
        inside = replies_ref[column, rows * slots + 8 * s : rows * slots + 8 * (s + 1), :]
        beyond = replies_ref[lax.rem(column + 1, peers), rows * slots + 8 * slots : rows * slots + 8 * slots + 8, :]
        halo = jnp.where(place == held - 1, beyond.astype(jnp.float32), inside.astype(jnp.float32))
        series = jnp.concatenate([block, halo], axis=0)

        def put(b, tile):
            ref_windows[LANES * b : LANES * (b + 1), :] = tile

        hankel_rows(lambda b: series[b : b + 1], rows + 1, put)
        centre, spread = window_stats(series)
        inverse = 1.0 / spread[:rows]
        weights[0, :, :] = inverse
        weights[1, :, :] = (M * centre[:rows]) * inverse
        start = region * block_len + lax.broadcasted_iota(jnp.int32, (rows, LANES), 0) * LANES + lane_iota(rows)
        weights[2, :, :] = jnp.where(start <= overall - M, 0.0, NEVER)
        running[...] = jnp.full(running.shape, NEVER, jnp.float32)

        def step(t, carry):
            j = pl.multiple_of(t * M, M)
            tile = jnp.concatenate([ref_windows[pl.ds(j, M), :], ref_windows[pl.ds(j + LANES, M), :]], axis=1)
            left = [jnp.broadcast_to(weights[k, pl.ds(2 * t, 1), :], (8, LANES)) for k in range(3)]
            right = [jnp.broadcast_to(weights[k, pl.ds(2 * t + 1, 1), :], (8, LANES)) for k in range(3)]
            for i in range(0, query_len, chunk):
                lhs = jnp.concatenate([windows_ref[s, i : i + chunk, :], windows_ref[s, i + LANES : i + LANES + chunk, :]], axis=1)
                products = jnp.dot(lhs, tile, preferred_element_type=jnp.float32)
                for r in range(0, chunk, 8):
                    mean = centre_ref[s, i + r : i + r + 8, :]
                    one = products[r : r + 8, :LANES] * left[0] - mean * left[1] + left[2]
                    two = products[r : r + 8, LANES:] * right[0] - mean * right[1] + right[2]
                    running[i + r : i + r + 8, :] = jnp.maximum(running[i + r : i + r + 8, :], jnp.maximum(one, two))
            return carry

        lax.fori_loop(0, block_len // M, step, 0)
        for b in range(query_len // LANES):
            best = jnp.max(running[LANES * b : LANES * (b + 1), :].T, axis=0, keepdims=True)
            best = best * scale_ref[s, b : b + 1, :]
            place_of = LANES * b + lane_iota(1)
            out_ref[s : s + 1, LANES * b : LANES * (b + 1)] = jnp.where(
                place_of <= lengths_ref[s] - M, 2.0 * (1.0 - best), 0.0
            )


VMEM = pl.BlockSpec(memory_space=pltpu.VMEM)
SMEM = pl.BlockSpec(memory_space=pltpu.SMEM)


def call(kernel, out_shape, in_specs, scratch=(), limit=8 << 20):
    many = isinstance(out_shape, tuple)
    return pl.pallas_call(
        kernel,
        out_shape=out_shape,
        in_specs=in_specs,
        out_specs=(VMEM,) * len(out_shape) if many else VMEM,
        scratch_shapes=scratch,
        compiler_params=pltpu.CompilerParams(vmem_limit_bytes=limit),
    )


def body(long_series, queries, lengths, groups):
    slots, query_len = queries.shape
    rows = long_series.shape[0] // LANES
    across, along = lax.axis_size("x"), lax.axis_size("y") * CORES
    overall = across * along * long_series.shape[0]
    asked = [groups] + [
        lax.ppermute(groups, "x", [(i, (i + d) % across) for i in range(across)]) for d in range(1, across)
    ]
    block = long_series.reshape(rows, LANES)
    gathered = lax.all_to_all(
        jnp.broadcast_to(block, (along, rows, LANES)), ("y", "core"), 0, 0, tiled=True
    )
    windows, centre, scale = call(
        prepare_queries,
        (
            jax.ShapeDtypeStruct((slots, query_len + LANES, LANES), jnp.bfloat16),
            jax.ShapeDtypeStruct((slots, query_len, LANES), jnp.float32),
            jax.ShapeDtypeStruct((slots, query_len // LANES, LANES), jnp.float32),
        ),
        [VMEM],
    )(queries)
    replies = call(
        answer,
        jax.ShapeDtypeStruct((across, rows * slots + 8 * slots + 8, LANES), jnp.bfloat16),
        [SMEM] * (1 + across) + [VMEM],
    )(lax.axis_index("x").reshape(1), *asked, gathered)
    received = lax.all_to_all(replies, "x", 0, 0, tiled=True)
    return call(
        functools.partial(join, along, overall),
        jax.ShapeDtypeStruct((slots, query_len), jnp.float32),
        [SMEM, SMEM, VMEM, VMEM, VMEM, VMEM],
        [
            pltpu.VMEM(((rows + 1) * LANES, LANES), jnp.bfloat16),
            pltpu.VMEM((3, rows, LANES), jnp.float32),
            pltpu.VMEM((query_len, LANES), jnp.float32),
        ],
    )(groups, lengths, received, windows, centre, scale)


def solution(mesh):
    outer, members = mesh.devices.shape
    side = math.isqrt(members // CORES)
    plane = Mesh(
        mesh.devices.reshape(outer, members // CORES // side, side, CORES), ("groups", "x", "y", "core")
    )
    every = ("groups", "x", "y", "core")
    return jax.shard_map(
        body,
        mesh=plane,
        in_specs=(P(every), P(every, None), P(every), P(every)),
        out_specs=P(every, None),
        check_vma=False,
    )
```

```python
import functools

import jax
import jax.numpy as jnp
from jax import lax
from jax.experimental import pallas as pl
from jax.experimental.pallas import tpu as pltpu
from jax.sharding import Mesh
from jax.sharding import PartitionSpec as P


M = 256
LANES = 128
SPREAD_FLOOR = 0.25
CORES = 2
NEVER = -3.0e38
PIECE = 64
LAG = 8


def lane_iota(rows):
    return lax.broadcasted_iota(jnp.int32, (rows, LANES), 1)


def ahead(x, n, width):
    rows = x.shape[0]
    below = pltpu.roll(x, rows - 1, axis=0)
    if n == width:
        return below
    lane = lane_iota(rows)
    return jnp.where(lane < width - n, pltpu.roll(x, width - n, axis=1), pltpu.roll(below, width - n, axis=1))


def window_stats(x):
    total = x
    squares = jnp.zeros_like(x)
    n = 1
    while n < M:
        other = ahead(total, n, LANES)
        apart = total - other
        squares = squares + apart * apart * (0.5 / n)
        if n > 1:
            squares = squares + ahead(merged, n, LANES)
        merged = squares
        total = total + other
        n *= 2
    centre = total * (1.0 / M)
    spread = jnp.sqrt(squares * (1.0 / M) + SPREAD_FLOOR)
    return centre, spread


class Hankel:
    def __init__(self, rows_of):
        self.rows_of = rows_of
        self.sub = lax.broadcasted_iota(jnp.int32, (8, LANES), 0)
        self.lane = lane_iota(8)
        self.kept = {}

    def rolled(self, b):
        if b not in self.kept:
            base = jnp.broadcast_to(self.rows_of(b), (8, LANES))
            for bit in (1, 2, 4):
                base = jnp.where((self.sub & bit) != 0, pltpu.roll(base, LANES - bit, axis=1), base)
            self.kept[b] = [base] + [pltpu.roll(base, LANES - 8 * t, axis=1) for t in range(1, LANES // 8)]
        return self.kept[b]

    def tile(self, b):
        own, after = self.rolled(b), self.rolled(b + 1)
        pieces = [
            jnp.where(self.lane + self.sub < LANES - 8 * t, own[t], after[t]) for t in range(LANES // 8)
        ]
        return jnp.concatenate(pieces, axis=0).astype(jnp.bfloat16)


def prepare_queries(queries_ref, windows_ref, centre_ref, scale_ref):
    count, length = queries_ref.shape
    rows = length // LANES
    zero = jnp.zeros((1, LANES), jnp.float32)
    for s in range(count):
        parts = [
            queries_ref[s : s + 1, LANES * b : LANES * (b + 1)].astype(jnp.float32)
            for b in range(rows)
        ]
        padded = parts + [zero] * 2
        hankel = Hankel(lambda b: padded[b])
        for b in range(rows + 1):
            windows_ref[s, LANES * b : LANES * (b + 1), :] = hankel.tile(b)
        series = jnp.concatenate(parts + [zero] * 8, axis=0)
        centre, spread = window_stats(series)
        scale_ref[s] = 1.0 / (M * spread[:rows])
        for b in range(rows):
            wide = jnp.broadcast_to(centre[b : b + 1], (LANES, LANES))
            centre_ref[s, LANES * b : LANES * (b + 1), :] = wide.T


def pick(theirs_ref, gathered_ref, out_ref):
    held, rows, _ = gathered_ref.shape
    slots = theirs_ref.shape[0]
    for s in range(slots):
        want = theirs_ref[s]
        out_ref[rows * s : rows * (s + 1), :] = gathered_ref[want // CORES]
        follow = jnp.minimum((want + 1) // CORES, held - 1)
        out_ref[rows * slots + 8 * s : rows * slots + 8 * (s + 1), :] = gathered_ref[follow, 0:8, :]


def join(overall, core_ref, groups_ref, lengths_ref, gathered_ref, passed_ref, windows_ref, centre_ref, scale_ref, out_ref, ref_windows, weights, running, series):
    held, rows, _ = gathered_ref.shape
    slots = groups_ref.shape[0]
    block_len = rows * LANES
    query_len = centre_ref.shape[1]
    parts = []
    for s in range(slots):
        region = groups_ref[s]
        follow = jnp.minimum((region + 1) // CORES, held - 1)
        block = jnp.where(
            lax.rem(region, CORES) == core_ref[0],
            gathered_ref[region // CORES].astype(jnp.float32),
            passed_ref[rows * s : rows * (s + 1), :].astype(jnp.float32),
        )
        halo = jnp.where(
            lax.rem(region + 1, CORES) == core_ref[0],
            gathered_ref[follow, 0:8, :].astype(jnp.float32),
            passed_ref[rows * slots + 8 * s : rows * slots + 8 * (s + 1), :].astype(jnp.float32),
        )
        parts.append(jnp.concatenate([block, halo], axis=0))
        series[s] = parts[s]
    centre, spread = window_stats(jnp.concatenate(parts, axis=0))
    inverse = 1.0 / spread
    factor = [inverse, (M * centre) * inverse]
    for s in range(slots):
        start = groups_ref[s] * block_len + LANES * lax.broadcasted_iota(jnp.int32, (rows + 8, LANES), 0) + lane_iota(rows + 8)
        for w in range(2):
            own = factor[w][(rows + 8) * s : (rows + 8) * (s + 1)]
            same = own[rows - M // LANES : rows - M // LANES + 1, 0:1]
            weights[w, (rows + 8) * s : (rows + 8) * (s + 1), :] = jnp.where(start <= overall - M, own, same)

    trips = block_len // (2 * M)
    pieces = query_len // PIECE
    tail = block_len - M

    def compute(*accs):
        def push(u):
            s, t = u // trips, u % trips
            for q in range(2):
                tile = []
                for h in range(2):
                    j = 2 * M * t + M * q + LANES * h
                    if q:
                        j = jnp.where(t == trips - 1, block_len + LANES + M * h, j)
                    tile.append(ref_windows[s, pl.ds(pl.multiple_of(j, LANES), M), :])
                pltpu.matmul_push_rhs(jnp.concatenate(tile, axis=1), staging_register=0, mxu_index=q)

        def factors(u):
            top = (rows + 8) * (u // trips) + 4 * (u % trips)
            return [
                [jnp.broadcast_to(weights[w, pl.ds(top + k, 1), :], (8, LANES)) for k in range(4)] for w in range(2)
            ]

        def drain(u, n, scale, shift):
            s = u // trips
            both = [pltpu.matmul_pop(accs[2 * n + q]) for q in range(2)]
            for r in range(0, PIECE, 8):
                at = PIECE * n + r
                mean = centre_ref[s, at : at + 8, :]
                found = [
                    both[k // 2][r : r + 8, LANES * (k % 2) : LANES * (k % 2 + 1)] * scale[k] - mean * shift[k]
                    for k in range(4)
                ]
                best = jnp.maximum(jnp.maximum(found[0], found[1]), jnp.maximum(found[2], found[3]))
                running[s, at : at + 8, :] = jnp.maximum(running[s, at : at + 8, :], best)

        def trip(u, first, last):
            s = u // trips
            before = None if first else factors(u - 1)
            now = factors(u)
            for n in range(pieces):
                i = PIECE * n
                lhs = jnp.concatenate(
                    [windows_ref[s, i : i + PIECE, :], windows_ref[s, i + LANES : i + LANES + PIECE, :]], axis=1
                )
                if n >= LAG:
                    drain(u, n - LAG, *now)
                elif not first:
                    drain(u - 1, pieces + n - LAG, *before)
                for q in range(2):
                    pltpu.matmul_acc_lhs(accs[2 * n + q], lhs, load_staged_rhs=0 if n == 0 else None)
                if n == 0 and not last:
                    push(u + 1)
            if last:
                for n in range(pieces - LAG, pieces):
                    drain(u, n, *now)

        for acc in accs:
            pltpu.matmul_pop(acc)
        push(0)
        trip(0, True, False)

        def middle(u, carry):
            trip(u, False, False)
            return carry

        lax.fori_loop(1, slots * trips - 1, middle, 0)
        trip(slots * trips - 1, False, True)

    running[...] = jnp.full(running.shape, NEVER, jnp.float32)
    for s in range(slots):
        hankel = Hankel(lambda b: series[s, b : b + 1, :])
        for b in range(rows + 1):
            tile = hankel.tile(b)
            ref_windows[s, LANES * b : LANES * (b + 1), :] = tile
            for h in range(4):
                if LANES * (b - h + h // 2) == tail:
                    at = block_len + LANES * (h + 1)
                    ref_windows[s, at : at + LANES, :] = tile
    for s in range(slots):

        @pl.when(groups_ref[s] * block_len + tail + LANES > overall - M)
        def _(s=s):
            for h in range(4):
                row = series[s, tail // LANES + h % 2 : tail // LANES + h % 2 + 1, :]
                same = jnp.broadcast_to(row, (LANES, LANES)).T.astype(jnp.bfloat16)
                at = block_len + LANES * (h + 1)
                ref_windows[s, at : at + LANES, :] = same

    pl.run_scoped(
        compute,
        *[pltpu.ACC(n % 2)((PIECE, 2 * LANES), jnp.float32) for n in range(2 * pieces)],
    )
    for s in range(slots):
        for b in range(query_len // LANES):
            best = jnp.max(running[s, LANES * b : LANES * (b + 1), :].T, axis=0, keepdims=True)
            best = best * scale_ref[s, b : b + 1, :]
            place_of = LANES * b + lane_iota(1)
            out_ref[s : s + 1, LANES * b : LANES * (b + 1)] = jnp.where(
                place_of <= lengths_ref[s] - M, 2.0 * (1.0 - best), 0.0
            )


VMEM = pl.BlockSpec(memory_space=pltpu.VMEM)
SMEM = pl.BlockSpec(memory_space=pltpu.SMEM)


def call(kernel, out_shape, in_specs, scratch=(), limit=12 << 20):
    many = isinstance(out_shape, tuple)
    return pl.pallas_call(
        kernel,
        out_shape=out_shape,
        in_specs=in_specs,
        out_specs=(VMEM,) * len(out_shape) if many else VMEM,
        scratch_shapes=scratch,
        compiler_params=pltpu.CompilerParams(vmem_limit_bytes=limit),
    )


def body(long_series, queries, lengths, groups):
    slots, query_len = queries.shape
    rows = long_series.shape[0] // LANES
    chips = lax.axis_size("chip")
    overall = chips * CORES * long_series.shape[0]
    swap = [(0, 1), (1, 0)]
    block = long_series.reshape(rows, LANES)
    gathered = lax.all_to_all(jnp.broadcast_to(block, (chips, rows, LANES)), "chip", 0, 0, tiled=True)
    theirs = lax.ppermute(groups, "core", swap)
    windows, centre, scale = call(
        prepare_queries,
        (
            jax.ShapeDtypeStruct((slots, query_len + LANES, LANES), jnp.bfloat16),
            jax.ShapeDtypeStruct((slots, query_len, LANES), jnp.float32),
            jax.ShapeDtypeStruct((slots, query_len // LANES, LANES), jnp.float32),
        ),
        [VMEM],
    )(queries)
    picked = call(pick, jax.ShapeDtypeStruct(((rows + 8) * slots, LANES), jnp.bfloat16), [SMEM, VMEM])(theirs, gathered)
    passed = lax.ppermute(picked, "core", swap)
    return call(
        functools.partial(join, overall),
        jax.ShapeDtypeStruct((slots, query_len), jnp.float32),
        [SMEM, SMEM, SMEM, VMEM, VMEM, VMEM, VMEM, VMEM],
        [
            pltpu.VMEM((slots, (rows + 5) * LANES, LANES), jnp.bfloat16),
            pltpu.VMEM((2, slots * (rows + 8), LANES), jnp.float32),
            pltpu.VMEM((slots, query_len, LANES), jnp.float32),
            pltpu.VMEM((slots, rows + 8, LANES), jnp.float32),
        ],
    )(lax.axis_index("core").reshape(1), groups, lengths, gathered, passed, windows, centre, scale)


def solution(mesh):
    outer, members = mesh.devices.shape
    pairs = Mesh(mesh.devices.reshape(outer, members // CORES, CORES), ("groups", "chip", "core"))
    every = ("groups", "chip", "core")
    return jax.shard_map(
        body,
        mesh=pairs,
        in_specs=(P(every), P(every, None), P(every), P(every)),
        out_specs=P(every, None),
        check_vma=False,
    )
```

```python
import functools

import jax
import jax.numpy as jnp
from jax import lax
from jax.experimental import pallas as pl
from jax.experimental.pallas import tpu as pltpu
from jax.sharding import Mesh
from jax.sharding import PartitionSpec as P


M = 256
LANES = 128
SPREAD_FLOOR = 0.25
CORES = 2
NEVER = -3.0e38
PIECE = 64
LAG = 8


def lane_iota(rows):
    return lax.broadcasted_iota(jnp.int32, (rows, LANES), 1)


def ahead(x, n, width):
    rows = x.shape[0]
    below = pltpu.roll(x, rows - 1, axis=0)
    if n == width:
        return below
    lane = lane_iota(rows)
    return jnp.where(lane < width - n, pltpu.roll(x, width - n, axis=1), pltpu.roll(below, width - n, axis=1))


def window_stats(x):
    total = x
    squares = jnp.zeros_like(x)
    n = 1
    while n < M:
        other = ahead(total, n, LANES)
        apart = total - other
        squares = squares + apart * apart * (0.5 / n)
        if n > 1:
            squares = squares + ahead(merged, n, LANES)
        merged = squares
        total = total + other
        n *= 2
    centre = total * (1.0 / M)
    spread = jnp.sqrt(squares * (1.0 / M) + SPREAD_FLOOR)
    return centre, spread


def sheared(row, shift):
    return pltpu.roll(jnp.broadcast_to(row, (LANES, LANES)), shift, axis=1, stride=1, stride_axis=0)


def prepare_queries(lengths_ref, queries_ref, turned_ref, windows_ref, centre_ref, ends_ref):
    count, length = queries_ref.shape
    rows = length // LANES
    zero = jnp.zeros((1, LANES), jnp.float32)
    upper = lane_iota(LANES) >= lax.broadcasted_iota(jnp.int32, (LANES, LANES), 0)
    place = LANES * lax.broadcasted_iota(jnp.int32, (rows, LANES), 0) + lane_iota(rows)
    for s in range(count):
        parts = [
            queries_ref[s : s + 1, LANES * b : LANES * (b + 1)].astype(jnp.float32)
            for b in range(rows)
        ]
        turned = [turned_ref[s : s + 1, length - LANES * (b + 1) : length - LANES * b] for b in range(rows)]
        turned = [sheared(row.astype(jnp.float32), 0) for row in turned] + [jnp.zeros((LANES, LANES), jnp.float32)] * 2
        for b in range(rows + 1):
            tile = jnp.where(upper, turned[b], turned[b + 1])
            windows_ref[s, LANES * b : LANES * (b + 1), :] = tile.astype(jnp.bfloat16)
        series = jnp.concatenate(parts + [zero] * 8, axis=0)
        centre, spread = window_stats(series)
        live = place <= lengths_ref[s] - M
        ends_ref[0, s] = jnp.where(live, 2.0, 0.0)
        ends_ref[1, s] = jnp.where(live, 2.0 / (M * spread[:rows]), 0.0)
        for b in range(rows):
            wide = jnp.broadcast_to(centre[b : b + 1], (LANES, LANES))
            centre_ref[s, LANES * b : LANES * (b + 1), :] = wide.T


def pick(theirs_ref, gathered_ref, out_ref):
    held, rows, _ = gathered_ref.shape
    slots = theirs_ref.shape[0]
    for s in range(slots):
        want = theirs_ref[s]
        out_ref[rows * s : rows * (s + 1), :] = gathered_ref[want // CORES]
        follow = jnp.minimum((want + 1) // CORES, held - 1)
        out_ref[rows * slots + 8 * s : rows * slots + 8 * (s + 1), :] = gathered_ref[follow, 0:8, :]


def join(overall, core_ref, groups_ref, gathered_ref, passed_ref, windows_ref, centre_ref, ends_ref, out_ref, ref_windows, weights, running, series):
    held, rows, _ = gathered_ref.shape
    slots = groups_ref.shape[0]
    block_len = rows * LANES
    query_len = centre_ref.shape[1]
    tail = rows - M // LANES
    parts = []
    for s in range(slots):
        region = groups_ref[s]
        follow = jnp.minimum((region + 1) // CORES, held - 1)
        block = jnp.where(
            lax.rem(region, CORES) == core_ref[0],
            gathered_ref[region // CORES].astype(jnp.float32),
            passed_ref[rows * s : rows * (s + 1), :].astype(jnp.float32),
        )
        halo = jnp.where(
            lax.rem(region + 1, CORES) == core_ref[0],
            gathered_ref[follow, 0:8, :].astype(jnp.float32),
            passed_ref[rows * slots + 8 * s : rows * slots + 8 * (s + 1), :].astype(jnp.float32),
        )
        parts.append(jnp.concatenate([block, halo], axis=0))
    every = jnp.concatenate(parts, axis=0)
    later = ahead(every, 1, LANES)
    centre, spread = window_stats(every)
    inverse = 1.0 / spread
    factors = [inverse, (M * centre) * inverse]
    for s in range(slots):
        first = (rows + 8) * s
        ends = groups_ref[s] * block_len + block_len > overall - M

        def moved(x, x_later, count):
            early = x_later[first + tail - 2 : first + tail - 2 + count]
            return jnp.where(ends, early, x[first + tail : first + tail + count])

        series[s, :rows, :] = every[first : first + rows]
        series[s, rows : rows + 4, :] = moved(every, later, 4)
        for w in range(2):
            weights[w, first : first + tail, :] = factors[w][first : first + tail]
            weights[w, first + tail : first + rows, :] = moved(factors[w], ahead(factors[w], 1, LANES), 2)
    trips = block_len // (2 * M)
    lines = (rows + 2) * LANES
    pieces = query_len // PIECE

    def compute(*accs):
        def push(u):
            s, t = u // trips, u % trips
            for q in range(2):
                j = lines - M - 2 * M * t - M * q
                if q:
                    j = j - jnp.where(t == trips - 1, LANES, 0)
                tile = [ref_windows[s, pl.ds(pl.multiple_of(j - LANES * h, LANES), M), :] for h in range(2)]
                pltpu.matmul_push_rhs(jnp.concatenate(tile, axis=1), staging_register=0, mxu_index=q)

        def rows_at(u):
            top = (rows + 8) * (u // trips) + 4 * (u % trips)
            return [
                [jnp.broadcast_to(weights[w, pl.ds(top + k, 1), :], (8, LANES)) for k in range(4)] for w in range(2)
            ]

        def drain(u, n, scale, shift):
            s = u // trips
            both = [pltpu.matmul_pop(accs[2 * n + q]) for q in range(2)]
            for r in range(0, PIECE, 8):
                at = PIECE * n + r
                mean = centre_ref[s, at : at + 8, :]
                found = [
                    both[k // 2][r : r + 8, LANES * (k % 2) : LANES * (k % 2 + 1)] * scale[k] - mean * shift[k]
                    for k in range(4)
                ]
                best = jnp.maximum(jnp.maximum(found[0], found[1]), jnp.maximum(found[2], found[3]))
                running[s, at : at + 8, :] = jnp.maximum(running[s, at : at + 8, :], best)

        def trip(u, first, last):
            s = u // trips
            before = None if first else rows_at(u - 1)
            now = rows_at(u)
            for n in range(pieces):
                i = PIECE * n
                lhs = jnp.concatenate(
                    [windows_ref[s, i + LANES : i + LANES + PIECE, :], windows_ref[s, i : i + PIECE, :]], axis=1
                )
                if n >= LAG:
                    drain(u, n - LAG, *now)
                elif not first:
                    drain(u - 1, pieces + n - LAG, *before)
                for q in range(2):
                    pltpu.matmul_acc_lhs(accs[2 * n + q], lhs, load_staged_rhs=0 if n == 0 else None)
                if n == 0 and not last:
                    push(u + 1)
            if last:
                for n in range(pieces - LAG, pieces):
                    drain(u, n, *now)

        for acc in accs:
            pltpu.matmul_pop(acc)
        push(0)
        trip(0, True, False)

        def middle(u, carry):
            trip(u, False, False)
            return carry

        lax.fori_loop(1, slots * trips - 1, middle, 0)
        trip(slots * trips - 1, False, True)

    running[...] = jnp.full(running.shape, NEVER, jnp.float32)
    lower = lane_iota(LANES) <= lax.broadcasted_iota(jnp.int32, (LANES, LANES), 0)
    own = [None] * slots
    for b in range(rows + 4):
        for s in range(slots):
            after = sheared(series[s, b : b + 1, :], 1)
            if b not in (0, rows):
                at = lines - LANES * (b - b // rows)
                ref_windows[s, at : at + LANES, :] = jnp.where(lower, own[s], after).astype(jnp.bfloat16)
            own[s] = after

    pl.run_scoped(
        compute,
        *[pltpu.ACC(n % 2)((PIECE, 2 * LANES), jnp.float32) for n in range(2 * pieces)],
    )
    for s in range(slots):
        for b in range(query_len // LANES):
            best = jnp.max(running[s, LANES * b : LANES * (b + 1), :].T, axis=0, keepdims=True)
            out_ref[s : s + 1, LANES * b : LANES * (b + 1)] = (
                ends_ref[0, s, b : b + 1, :] - best * ends_ref[1, s, b : b + 1, :]
            )


VMEM = pl.BlockSpec(memory_space=pltpu.VMEM)
SMEM = pl.BlockSpec(memory_space=pltpu.SMEM)


def call(kernel, out_shape, in_specs, scratch=(), limit=12 << 20):
    many = isinstance(out_shape, tuple)
    return pl.pallas_call(
        kernel,
        out_shape=out_shape,
        in_specs=in_specs,
        out_specs=(VMEM,) * len(out_shape) if many else VMEM,
        scratch_shapes=scratch,
        compiler_params=pltpu.CompilerParams(vmem_limit_bytes=limit),
    )


def prepare_call(slots, query_len):
    return call(
        prepare_queries,
        (
            jax.ShapeDtypeStruct((slots, query_len + LANES, LANES), jnp.bfloat16),
            jax.ShapeDtypeStruct((slots, query_len, LANES), jnp.float32),
            jax.ShapeDtypeStruct((2, slots, query_len // LANES, LANES), jnp.float32),
        ),
        [SMEM, VMEM, VMEM],
    )


def join_call(slots, rows, query_len, overall):
    return call(
        functools.partial(join, overall),
        jax.ShapeDtypeStruct((slots, query_len), jnp.float32),
        [SMEM, SMEM, VMEM, VMEM, VMEM, VMEM, VMEM],
        [
            pltpu.VMEM((slots, (rows + 2) * LANES, LANES), jnp.bfloat16),
            pltpu.VMEM((2, slots * (rows + 8), LANES), jnp.float32),
            pltpu.VMEM((slots, query_len, LANES), jnp.float32),
            pltpu.VMEM((slots, rows + 8, LANES), jnp.float32),
        ],
    )


def body(long_series, queries, lengths, groups):
    slots, query_len = queries.shape
    rows = long_series.shape[0] // LANES
    chips = lax.axis_size("chip")
    overall = chips * CORES * long_series.shape[0]
    swap = [(0, 1), (1, 0)]
    block = long_series.reshape(rows, LANES)
    gathered = lax.all_to_all(jnp.broadcast_to(block, (chips, rows, LANES)), "chip", 0, 0, tiled=True)
    theirs = lax.ppermute(groups, "core", swap)
    windows, centre, ends = prepare_call(slots, query_len)(lengths, queries, queries[:, ::-1])
    picked = call(pick, jax.ShapeDtypeStruct(((rows + 8) * slots, LANES), jnp.bfloat16), [SMEM, VMEM])(theirs, gathered)
    passed = lax.ppermute(picked, "core", swap)
    core = lax.axis_index("core").reshape(1)
    return join_call(slots, rows, query_len, overall)(core, groups, gathered, passed, windows, centre, ends)


def solution(mesh):
    outer, members = mesh.devices.shape
    pairs = Mesh(mesh.devices.reshape(outer, members // CORES, CORES), ("groups", "chip", "core"))
    every = ("groups", "chip", "core")
    return jax.shard_map(
        body,
        mesh=pairs,
        in_specs=(P(every), P(every, None), P(every), P(every)),
        out_specs=P(every, None),
        check_vma=False,
    )
```

```python
import functools

import jax
import jax.numpy as jnp
from jax import lax
from jax.experimental import pallas as pl
from jax.experimental.pallas import tpu as pltpu
from jax.sharding import Mesh
from jax.sharding import PartitionSpec as P


M = 256
LANES = 128
SPREAD_FLOOR = 0.25
CORES = 2
NEVER = -3.0e38
PIECE = 128
LAG = 3


def lane_iota(rows):
    return lax.broadcasted_iota(jnp.int32, (rows, LANES), 1)


def ahead(x, n):
    rows = x.shape[0]
    if n % LANES == 0:
        return pltpu.roll(x, rows - n // LANES, axis=0)
    turned = pltpu.roll(x, LANES - n % LANES, axis=1)
    below = pltpu.roll(turned, rows - n // LANES - 1, axis=0)
    if n >= LANES:
        turned = pltpu.roll(turned, rows - n // LANES, axis=0)
    return jnp.where(lane_iota(rows) < LANES - n % LANES, turned, below)


def window_stats(x):
    total, squares, n = x, None, 1
    while n < M:
        sums = [total] + [ahead(total, n * k) for k in range(1, 4)]
        whole = (sums[0] + sums[1]) + (sums[2] + sums[3])
        apart = [(piece - whole * 0.25) for piece in sums]
        spare = ((apart[0] * apart[0] + apart[1] * apart[1]) + (apart[2] * apart[2] + apart[3] * apart[3])) * (1.0 / n)
        if n > 1:
            kept = [squares] + [ahead(squares, n * k) for k in range(1, 4)]
            spare = spare + ((kept[0] + kept[1]) + (kept[2] + kept[3]))
        total, squares = whole, spare
        n *= 4
    centre = total * (1.0 / M)
    spread = jnp.sqrt(squares * (1.0 / M) + SPREAD_FLOOR)
    return centre, spread


def sheared(row, shift):
    return pltpu.roll(jnp.broadcast_to(row, (LANES, LANES)), shift, axis=1, stride=1, stride_axis=0)


def prepare_queries(lengths_ref, queries_ref, turned_ref, windows_ref, centre_ref, ends_ref):
    count, length = queries_ref.shape
    rows = length // LANES
    zero = jnp.zeros((1, LANES), jnp.float32)
    upper = lane_iota(LANES) >= lax.broadcasted_iota(jnp.int32, (LANES, LANES), 0)
    place = LANES * lax.broadcasted_iota(jnp.int32, (rows, LANES), 0) + lane_iota(rows)
    for s in range(count):
        parts = [
            queries_ref[s : s + 1, LANES * b : LANES * (b + 1)].astype(jnp.float32)
            for b in range(rows)
        ]
        turned = [turned_ref[s : s + 1, length - LANES * (b + 1) : length - LANES * b] for b in range(rows)]
        turned = [sheared(row.astype(jnp.float32), 0) for row in turned] + [jnp.zeros((LANES, LANES), jnp.float32)] * 2
        for b in range(rows + 1):
            tile = jnp.where(upper, turned[b], turned[b + 1])
            windows_ref[s, LANES * b : LANES * (b + 1), :] = tile.astype(jnp.bfloat16)
        series = jnp.concatenate(parts + [zero] * 8, axis=0)
        centre, spread = window_stats(series)
        live = place <= lengths_ref[s] - M
        ends_ref[0, s] = jnp.where(live, 2.0, 0.0)
        ends_ref[1, s] = jnp.where(live, 2.0 / (M * spread[:rows]), 0.0)
        for b in range(rows):
            wide = jnp.broadcast_to(centre[b : b + 1], (LANES, LANES))
            centre_ref[s, LANES * b : LANES * (b + 1), :] = wide.T


def pick(theirs_ref, gathered_ref, out_ref):
    held, rows, _ = gathered_ref.shape
    slots = theirs_ref.shape[0]
    for s in range(slots):
        want = theirs_ref[s]
        out_ref[rows * s : rows * (s + 1), :] = gathered_ref[want // CORES]
        follow = jnp.minimum((want + 1) // CORES, held - 1)
        out_ref[rows * slots + 8 * s : rows * slots + 8 * (s + 1), :] = gathered_ref[follow, 0:8, :]


def join(overall, core_ref, groups_ref, gathered_ref, passed_ref, windows_ref, centre_ref, ends_ref, out_ref, ref_windows, weights, running, series):
    held, rows, _ = gathered_ref.shape
    slots = groups_ref.shape[0]
    block_len = rows * LANES
    query_len = centre_ref.shape[1]
    tail = rows - M // LANES
    parts = []
    for s in range(slots):
        region = groups_ref[s]
        follow = jnp.minimum((region + 1) // CORES, held - 1)
        block = jnp.where(
            lax.rem(region, CORES) == core_ref[0],
            gathered_ref[region // CORES].astype(jnp.float32),
            passed_ref[rows * s : rows * (s + 1), :].astype(jnp.float32),
        )
        halo = jnp.where(
            lax.rem(region + 1, CORES) == core_ref[0],
            gathered_ref[follow, 0:8, :].astype(jnp.float32),
            passed_ref[rows * slots + 8 * s : rows * slots + 8 * (s + 1), :].astype(jnp.float32),
        )
        parts.append(jnp.concatenate([block, halo], axis=0))
    every = jnp.concatenate(parts, axis=0)
    later = ahead(every, 1)
    centre, spread = window_stats(every)
    inverse = 1.0 / spread
    factors = [inverse, (M * centre) * inverse]
    for s in range(slots):
        first = (rows + 8) * s
        ends = groups_ref[s] * block_len + block_len > overall - M

        def moved(x, x_later, count):
            early = x_later[first + tail - 2 : first + tail - 2 + count]
            return jnp.where(ends, early, x[first + tail : first + tail + count])

        series[s, :rows, :] = every[first : first + rows]
        series[s, rows : rows + 4, :] = moved(every, later, 4)
        for w in range(2):
            weights[w, first : first + tail, :] = factors[w][first : first + tail]
            weights[w, first + tail : first + rows, :] = moved(factors[w], ahead(factors[w], 1), 2)
    lower = lane_iota(LANES) <= lax.broadcasted_iota(jnp.int32, (LANES, LANES), 0)
    own = [None] * slots

    def build(s, b):
        after = sheared(series[s, b : b + 1, :], 1)
        if b not in (0, rows):
            at = lines - LANES * (b - b // rows)
            ref_windows[s, at : at + LANES, :] = jnp.where(lower, own[s], after).astype(jnp.bfloat16)
        own[s] = after

    def finish(s, b):
        best = jnp.max(running[s, LANES * b : LANES * (b + 1), :].T, axis=0, keepdims=True)
        out_ref[s : s + 1, LANES * b : LANES * (b + 1)] = (
            ends_ref[0, s, b : b + 1, :] - best * ends_ref[1, s, b : b + 1, :]
        )

    trips = block_len // (2 * M)
    lines = (rows + 2) * LANES
    pieces = query_len // PIECE

    def compute(*accs):
        def push(u):
            s, t = u // trips, u % trips
            for q in range(2):
                j = lines - M - 2 * M * t - M * q
                if q:
                    j = j - jnp.where(t == trips - 1, LANES, 0)
                tile = [ref_windows[s, pl.ds(pl.multiple_of(j - LANES * h, LANES), M), :] for h in range(2)]
                pltpu.matmul_push_rhs(jnp.concatenate(tile, axis=1), staging_register=0, mxu_index=q)

        def rows_at(u):
            top = (rows + 8) * (u // trips) + 4 * (u % trips)
            return [
                [jnp.broadcast_to(weights[w, pl.ds(top + k, 1), :], (8, LANES)) for k in range(4)] for w in range(2)
            ]

        def drain(u, n, scale, shift):
            s = u // trips
            both = [pltpu.matmul_pop(accs[2 * n + q]) for q in range(2)]
            for r in range(0, PIECE, 8):
                at = PIECE * n + r
                mean = centre_ref[s, at : at + 8, :]
                found = [
                    both[k // 2][r : r + 8, LANES * (k % 2) : LANES * (k % 2 + 1)] * scale[k] - mean * shift[k]
                    for k in range(4)
                ]
                best = jnp.maximum(jnp.maximum(found[0], found[1]), jnp.maximum(found[2], found[3]))
                running[s, at : at + 8, :] = jnp.maximum(running[s, at : at + 8, :], best)

        def trip(u, first, last, extras=()):
            s = u // trips
            extras = list(extras)
            share = -(-len(extras) // pieces)
            before = None if first else rows_at(u - 1)
            now = rows_at(u)
            for n in range(pieces):
                i = PIECE * n
                lhs = jnp.concatenate(
                    [windows_ref[s, i + LANES : i + LANES + PIECE, :], windows_ref[s, i : i + PIECE, :]], axis=1
                )
                if n >= LAG:
                    drain(u, n - LAG, *now)
                elif not first:
                    drain(u - 1, pieces + n - LAG, *before)
                for q in range(2):
                    pltpu.matmul_acc_lhs(accs[2 * n + q], lhs, load_staged_rhs=0 if n == 0 else None)
                for extra in extras[share * n : share * (n + 1)]:
                    extra()
                if n == (pieces - 2 if first else 0) and not last:
                    push(u + 1)
            if last:
                for n in range(pieces - LAG, pieces):
                    drain(u, n, *now)

        for acc in accs:
            pltpu.matmul_pop(acc)
        order = [(s, b) for s in range(slots) for b in range(rows + 4)]
        early = 2 * M // LANES + 2
        for s, b in order[:early]:
            build(s, b)
        push(0)
        trip(0, True, False, [functools.partial(build, s, b) for s, b in order[early:]])

        def middle(u, carry):
            trip(u, False, False)
            return carry

        lax.fori_loop(1, slots * trips - 1, middle, 0)
        done = [(s, b) for s in range(slots - 1) for b in range(query_len // LANES)]
        trip(slots * trips - 1, False, True, [functools.partial(finish, s, b) for s, b in done])
        for b in range(query_len // LANES):
            finish(slots - 1, b)

    running[...] = jnp.full(running.shape, NEVER, jnp.float32)
    pl.run_scoped(
        compute,
        *[pltpu.ACC(n % 2)((PIECE, 2 * LANES), jnp.float32) for n in range(2 * pieces)],
    )


VMEM = pl.BlockSpec(memory_space=pltpu.VMEM)
SMEM = pl.BlockSpec(memory_space=pltpu.SMEM)


def call(kernel, out_shape, in_specs, scratch=(), limit=12 << 20):
    many = isinstance(out_shape, tuple)
    return pl.pallas_call(
        kernel,
        out_shape=out_shape,
        in_specs=in_specs,
        out_specs=(VMEM,) * len(out_shape) if many else VMEM,
        scratch_shapes=scratch,
        compiler_params=pltpu.CompilerParams(vmem_limit_bytes=limit),
    )


def prepare_call(slots, query_len):
    return call(
        prepare_queries,
        (
            jax.ShapeDtypeStruct((slots, query_len + LANES, LANES), jnp.bfloat16),
            jax.ShapeDtypeStruct((slots, query_len, LANES), jnp.float32),
            jax.ShapeDtypeStruct((2, slots, query_len // LANES, LANES), jnp.float32),
        ),
        [SMEM, VMEM, VMEM],
    )


def join_call(slots, rows, query_len, overall):
    return call(
        functools.partial(join, overall),
        jax.ShapeDtypeStruct((slots, query_len), jnp.float32),
        [SMEM, SMEM, VMEM, VMEM, VMEM, VMEM, VMEM],
        [
            pltpu.VMEM((slots, (rows + 2) * LANES, LANES), jnp.bfloat16),
            pltpu.VMEM((2, slots * (rows + 8), LANES), jnp.float32),
            pltpu.VMEM((slots, query_len, LANES), jnp.float32),
            pltpu.VMEM((slots, rows + 8, LANES), jnp.float32),
        ],
    )


def body(long_series, queries, lengths, groups):
    slots, query_len = queries.shape
    rows = long_series.shape[0] // LANES
    chips = lax.axis_size("chip")
    overall = chips * CORES * long_series.shape[0]
    swap = [(0, 1), (1, 0)]
    block = long_series.reshape(rows, LANES)
    gathered = lax.all_to_all(jnp.broadcast_to(block, (chips, rows, LANES)), "chip", 0, 0, tiled=True)
    theirs = lax.ppermute(groups, "core", swap)
    windows, centre, ends = prepare_call(slots, query_len)(lengths, queries, queries[:, ::-1])
    picked = call(pick, jax.ShapeDtypeStruct(((rows + 8) * slots, LANES), jnp.bfloat16), [SMEM, VMEM])(theirs, gathered)
    passed = lax.ppermute(picked, "core", swap)
    core = lax.axis_index("core").reshape(1)
    return join_call(slots, rows, query_len, overall)(core, groups, gathered, passed, windows, centre, ends)


def solution(mesh):
    outer, members = mesh.devices.shape
    pairs = Mesh(mesh.devices.reshape(outer, members // CORES, CORES), ("groups", "chip", "core"))
    every = ("groups", "chip", "core")
    return jax.shard_map(
        body,
        mesh=pairs,
        in_specs=(P(every), P(every, None), P(every), P(every)),
        out_specs=P(every, None),
        check_vma=False,
    )
```

```python
import functools

import jax
import jax.numpy as jnp
from jax import lax
from jax.experimental import pallas as pl
from jax.experimental.pallas import tpu as pltpu
from jax.sharding import Mesh
from jax.sharding import PartitionSpec as P


M = 256
LANES = 128
SPREAD_FLOOR = 0.25
CORES = 2
NEVER = -3.0e38
PIECE = 128
LAG = 3


def lane_iota(rows):
    return lax.broadcasted_iota(jnp.int32, (rows, LANES), 1)


def ahead(x, n):
    rows = x.shape[0]
    if n % LANES == 0:
        return pltpu.roll(x, rows - n // LANES, axis=0)
    turned = pltpu.roll(x, LANES - n % LANES, axis=1)
    below = pltpu.roll(turned, rows - n // LANES - 1, axis=0)
    if n >= LANES:
        turned = pltpu.roll(turned, rows - n // LANES, axis=0)
    return jnp.where(lane_iota(rows) < LANES - n % LANES, turned, below)


def window_stats(x):
    total, squares, n = x, None, 1
    while n < M:
        sums = [total] + [ahead(total, n * k) for k in range(1, 4)]
        whole = (sums[0] + sums[1]) + (sums[2] + sums[3])
        apart = [(piece - whole * 0.25) for piece in sums]
        spare = ((apart[0] * apart[0] + apart[1] * apart[1]) + (apart[2] * apart[2] + apart[3] * apart[3])) * (1.0 / n)
        if n > 1:
            kept = [squares] + [ahead(squares, n * k) for k in range(1, 4)]
            spare = spare + ((kept[0] + kept[1]) + (kept[2] + kept[3]))
        total, squares = whole, spare
        n *= 4
    centre = total * (1.0 / M)
    spread = jnp.sqrt(squares * (1.0 / M) + SPREAD_FLOOR)
    return centre, spread


def sheared(row, shift):
    return pltpu.roll(jnp.broadcast_to(row, (LANES, LANES)), shift, axis=1, stride=1, stride_axis=0)


def prepare_queries(lengths_ref, queries_ref, turned_ref, windows_ref, centre_ref, ends_ref):
    count, length = queries_ref.shape
    rows = length // LANES
    zero = jnp.zeros((1, LANES), jnp.float32)
    upper = lane_iota(LANES) >= lax.broadcasted_iota(jnp.int32, (LANES, LANES), 0)
    place = LANES * lax.broadcasted_iota(jnp.int32, (rows, LANES), 0) + lane_iota(rows)
    for s in range(count):
        parts = [
            queries_ref[s : s + 1, LANES * b : LANES * (b + 1)].astype(jnp.float32)
            for b in range(rows)
        ]
        turned = [turned_ref[s : s + 1, length - LANES * (b + 1) : length - LANES * b] for b in range(rows)]
        turned = [sheared(row.astype(jnp.float32), 0) for row in turned] + [jnp.zeros((LANES, LANES), jnp.float32)] * 2
        for b in range(rows + 1):
            tile = jnp.where(upper, turned[b], turned[b + 1])
            windows_ref[s, LANES * b : LANES * (b + 1), :] = tile.astype(jnp.bfloat16)
        series = jnp.concatenate(parts + [zero] * 8, axis=0)
        centre, spread = window_stats(series)
        live = place <= lengths_ref[s] - M
        ends_ref[0, s] = jnp.where(live, 2.0, 0.0)
        ends_ref[1, s] = jnp.where(live, 2.0 / (M * spread[:rows]), 0.0)
        for b in range(rows):
            wide = jnp.broadcast_to(centre[b : b + 1], (LANES, LANES))
            centre_ref[s, LANES * b : LANES * (b + 1), :] = wide.T


def spread(block_ref, out_ref, arrived):
    copies = [pltpu.make_async_copy(block_ref, out_ref.at[p], arrived.at[p]) for p in range(out_ref.shape[0])]
    for copy in copies:
        copy.start()
    for copy in copies:
        copy.wait()


def pick(theirs_ref, gathered_ref, out_ref):
    held, rows, _ = gathered_ref.shape
    slots = theirs_ref.shape[0]
    for s in range(slots):
        want = theirs_ref[s]
        out_ref[rows * s : rows * (s + 1), :] = gathered_ref[want // CORES]
        follow = jnp.minimum((want + 1) // CORES, held - 1)
        out_ref[rows * slots + 8 * s : rows * slots + 8 * (s + 1), :] = gathered_ref[follow, 0:8, :]


def join(overall, core_ref, groups_ref, gathered_ref, passed_ref, windows_ref, centre_ref, ends_ref, out_ref, ref_windows, weights, running, series):
    held, rows, _ = gathered_ref.shape
    slots = groups_ref.shape[0]
    block_len = rows * LANES
    query_len = centre_ref.shape[1]
    tail = rows - M // LANES
    parts = []
    for s in range(slots):
        region = groups_ref[s]
        follow = jnp.minimum((region + 1) // CORES, held - 1)
        block = jnp.where(
            lax.rem(region, CORES) == core_ref[0],
            gathered_ref[region // CORES].astype(jnp.float32),
            passed_ref[rows * s : rows * (s + 1), :].astype(jnp.float32),
        )
        halo = jnp.where(
            lax.rem(region + 1, CORES) == core_ref[0],
            gathered_ref[follow, 0:8, :].astype(jnp.float32),
            passed_ref[rows * slots + 8 * s : rows * slots + 8 * (s + 1), :].astype(jnp.float32),
        )
        parts.append(jnp.concatenate([block, halo], axis=0))
    every = jnp.concatenate(parts, axis=0)
    later = ahead(every, 1)
    centre, spread = window_stats(every)
    inverse = 1.0 / spread
    factors = [inverse, (M * centre) * inverse]
    for s in range(slots):
        first = (rows + 8) * s
        ends = groups_ref[s] * block_len + block_len > overall - M

        def moved(x, x_later, count):
            early = x_later[first + tail - 2 : first + tail - 2 + count]
            return jnp.where(ends, early, x[first + tail : first + tail + count])

        series[s, :rows, :] = every[first : first + rows]
        series[s, rows : rows + 4, :] = moved(every, later, 4)
        for w in range(2):
            weights[w, first : first + tail, :] = factors[w][first : first + tail]
            weights[w, first + tail : first + rows, :] = moved(factors[w], ahead(factors[w], 1), 2)
    lower = lane_iota(LANES) <= lax.broadcasted_iota(jnp.int32, (LANES, LANES), 0)
    own = [None] * slots

    def build(s, b):
        after = sheared(series[s, b : b + 1, :], 1)
        if b not in (0, rows):
            at = lines - LANES * (b - b // rows)
            ref_windows[s, at : at + LANES, :] = jnp.where(lower, own[s], after).astype(jnp.bfloat16)
        own[s] = after

    def finish(s, b):
        best = jnp.max(running[s, LANES * b : LANES * (b + 1), :].T, axis=0, keepdims=True)
        out_ref[s : s + 1, LANES * b : LANES * (b + 1)] = (
            ends_ref[0, s, b : b + 1, :] - best * ends_ref[1, s, b : b + 1, :]
        )

    trips = block_len // (2 * M)
    lines = (rows + 2) * LANES
    pieces = query_len // PIECE

    def compute(*accs):
        def push(u):
            s, t = u // trips, u % trips
            for q in range(2):
                j = lines - M - 2 * M * t - M * q
                if q:
                    j = j - jnp.where(t == trips - 1, LANES, 0)
                tile = [ref_windows[s, pl.ds(pl.multiple_of(j - LANES * h, LANES), M), :] for h in range(2)]
                pltpu.matmul_push_rhs(jnp.concatenate(tile, axis=1), staging_register=0, mxu_index=q)

        def rows_at(u):
            top = (rows + 8) * (u // trips) + 4 * (u % trips)
            return [
                [jnp.broadcast_to(weights[w, pl.ds(top + k, 1), :], (8, LANES)) for k in range(4)] for w in range(2)
            ]

        def drain(u, n, scale, shift):
            s = u // trips
            both = [pltpu.matmul_pop(accs[2 * n + q]) for q in range(2)]
            for r in range(0, PIECE, 8):
                at = PIECE * n + r
                mean = centre_ref[s, at : at + 8, :]
                found = [
                    both[k // 2][r : r + 8, LANES * (k % 2) : LANES * (k % 2 + 1)] * scale[k] - mean * shift[k]
                    for k in range(4)
                ]
                best = jnp.maximum(jnp.maximum(found[0], found[1]), jnp.maximum(found[2], found[3]))
                running[s, at : at + 8, :] = jnp.maximum(running[s, at : at + 8, :], best)

        def trip(u, first, last, extras=()):
            s = u // trips
            extras = list(extras)
            share = -(-len(extras) // pieces)
            before = None if first else rows_at(u - 1)
            now = rows_at(u)
            for n in range(pieces):
                i = PIECE * n
                lhs = jnp.concatenate(
                    [windows_ref[s, i + LANES : i + LANES + PIECE, :], windows_ref[s, i : i + PIECE, :]], axis=1
                )
                if n >= LAG:
                    drain(u, n - LAG, *now)
                elif not first:
                    drain(u - 1, pieces + n - LAG, *before)
                for q in range(2):
                    pltpu.matmul_acc_lhs(accs[2 * n + q], lhs, load_staged_rhs=0 if n == 0 else None)
                for extra in extras[share * n : share * (n + 1)]:
                    extra()
                if n == (pieces - 2 if first else 0) and not last:
                    push(u + 1)
            if last:
                for n in range(pieces - LAG, pieces):
                    drain(u, n, *now)

        for acc in accs:
            pltpu.matmul_pop(acc)
        order = [(s, b) for s in range(slots) for b in range(rows + 4)]
        early = 2 * M // LANES + 2
        for s, b in order[:early]:
            build(s, b)
        push(0)
        trip(0, True, False, [functools.partial(build, s, b) for s, b in order[early:]])

        def middle(u, carry):
            trip(u, False, False)
            return carry

        lax.fori_loop(1, slots * trips - 1, middle, 0)
        done = [(s, b) for s in range(slots - 1) for b in range(query_len // LANES)]
        trip(slots * trips - 1, False, True, [functools.partial(finish, s, b) for s, b in done])
        for b in range(query_len // LANES):
            finish(slots - 1, b)

    running[...] = jnp.full(running.shape, NEVER, jnp.float32)
    pl.run_scoped(
        compute,
        *[pltpu.ACC(n % 2)((PIECE, 2 * LANES), jnp.float32) for n in range(2 * pieces)],
    )


VMEM = pl.BlockSpec(memory_space=pltpu.VMEM)
SMEM = pl.BlockSpec(memory_space=pltpu.SMEM)


def call(kernel, out_shape, in_specs, scratch=(), limit=12 << 20):
    many = isinstance(out_shape, tuple)
    return pl.pallas_call(
        kernel,
        out_shape=out_shape,
        in_specs=in_specs,
        out_specs=(VMEM,) * len(out_shape) if many else VMEM,
        scratch_shapes=scratch,
        compiler_params=pltpu.CompilerParams(vmem_limit_bytes=limit),
    )


def prepare_call(slots, query_len):
    return call(
        prepare_queries,
        (
            jax.ShapeDtypeStruct((slots, query_len + LANES, LANES), jnp.bfloat16),
            jax.ShapeDtypeStruct((slots, query_len, LANES), jnp.float32),
            jax.ShapeDtypeStruct((2, slots, query_len // LANES, LANES), jnp.float32),
        ),
        [SMEM, VMEM, VMEM],
    )


def join_call(slots, rows, query_len, overall):
    return call(
        functools.partial(join, overall),
        jax.ShapeDtypeStruct((slots, query_len), jnp.float32),
        [SMEM, SMEM, VMEM, VMEM, VMEM, VMEM, VMEM],
        [
            pltpu.VMEM((slots, (rows + 2) * LANES, LANES), jnp.bfloat16),
            pltpu.VMEM((2, slots * (rows + 8), LANES), jnp.float32),
            pltpu.VMEM((slots, query_len, LANES), jnp.float32),
            pltpu.VMEM((slots, rows + 8, LANES), jnp.float32),
        ],
    )


def body(long_series, queries, lengths, groups):
    slots, query_len = queries.shape
    rows = long_series.shape[0] // LANES
    chips = lax.axis_size("chip")
    overall = chips * CORES * long_series.shape[0]
    swap = [(0, 1), (1, 0)]
    block = long_series.reshape(rows, LANES)
    copies = pl.pallas_call(
        spread,
        out_shape=jax.ShapeDtypeStruct((chips, rows, LANES), jnp.bfloat16),
        in_specs=[pl.BlockSpec(memory_space=pltpu.HBM)],
        out_specs=pl.BlockSpec(memory_space=pltpu.HBM),
        scratch_shapes=[pltpu.SemaphoreType.DMA((chips,))],
        name="spread",
    )(block)
    gathered = lax.all_to_all(copies, "chip", 0, 0, tiled=True)
    theirs = lax.ppermute(groups, "core", swap)
    windows, centre, ends = prepare_call(slots, query_len)(lengths, queries, queries[:, ::-1])
    picked = call(pick, jax.ShapeDtypeStruct(((rows + 8) * slots, LANES), jnp.bfloat16), [SMEM, VMEM])(theirs, gathered)
    passed = lax.ppermute(picked, "core", swap)
    core = lax.axis_index("core").reshape(1)
    return join_call(slots, rows, query_len, overall)(core, groups, gathered, passed, windows, centre, ends)


def solution(mesh):
    outer, members = mesh.devices.shape
    pairs = Mesh(mesh.devices.reshape(outer, members // CORES, CORES), ("groups", "chip", "core"))
    every = ("groups", "chip", "core")
    return jax.shard_map(
        body,
        mesh=pairs,
        in_specs=(P(every), P(every, None), P(every), P(every)),
        out_specs=P(every, None),
        check_vma=False,
    )
```

```python
import functools

import jax
import jax.numpy as jnp
from jax import lax
from jax.experimental import pallas as pl
from jax.experimental.pallas import tpu as pltpu
from jax.sharding import Mesh
from jax.sharding import PartitionSpec as P


M = 256
LANES = 128
SPREAD_FLOOR = 0.25
CORES = 2
NEVER = -3.0e38
PIECE = 128
LAG = 3


def lane_iota(rows):
    return lax.broadcasted_iota(jnp.int32, (rows, LANES), 1)


def ahead(x, n):
    rows = x.shape[0]
    if n % LANES == 0:
        return pltpu.roll(x, rows - n // LANES, axis=0)
    turned = pltpu.roll(x, LANES - n % LANES, axis=1)
    below = pltpu.roll(turned, rows - n // LANES - 1, axis=0)
    if n >= LANES:
        turned = pltpu.roll(turned, rows - n // LANES, axis=0)
    return jnp.where(lane_iota(rows) < LANES - n % LANES, turned, below)


def window_stats(x):
    total, squares, n = x, None, 1
    while n < M:
        sums = [total] + [ahead(total, n * k) for k in range(1, 4)]
        whole = (sums[0] + sums[1]) + (sums[2] + sums[3])
        apart = [(piece - whole * 0.25) for piece in sums]
        spare = ((apart[0] * apart[0] + apart[1] * apart[1]) + (apart[2] * apart[2] + apart[3] * apart[3])) * (1.0 / n)
        if n > 1:
            kept = [squares] + [ahead(squares, n * k) for k in range(1, 4)]
            spare = spare + ((kept[0] + kept[1]) + (kept[2] + kept[3]))
        total, squares = whole, spare
        n *= 4
    centre = total * (1.0 / M)
    spread = jnp.sqrt(squares * (1.0 / M) + SPREAD_FLOOR)
    return centre, spread


def sheared(row, shift):
    return pltpu.roll(jnp.broadcast_to(row, (LANES, LANES)), shift, axis=1, stride=1, stride_axis=0)


def prepare_queries(lengths_ref, queries_ref, turned_ref, windows_ref, centre_ref, ends_ref):
    count, length = queries_ref.shape
    rows = length // LANES
    zero = jnp.zeros((1, LANES), jnp.float32)
    upper = lane_iota(LANES) >= lax.broadcasted_iota(jnp.int32, (LANES, LANES), 0)
    place = LANES * lax.broadcasted_iota(jnp.int32, (rows, LANES), 0) + lane_iota(rows)
    for s in range(count):
        parts = [
            queries_ref[s : s + 1, LANES * b : LANES * (b + 1)].astype(jnp.float32)
            for b in range(rows)
        ]
        turned = [turned_ref[s : s + 1, length - LANES * (b + 1) : length - LANES * b] for b in range(rows)]
        turned = [sheared(row.astype(jnp.float32), 0) for row in turned] + [jnp.zeros((LANES, LANES), jnp.float32)] * 2
        for b in range(rows + 1):
            tile = jnp.where(upper, turned[b], turned[b + 1])
            windows_ref[s, LANES * b : LANES * (b + 1), :] = tile.astype(jnp.bfloat16)
        series = jnp.concatenate(parts + [zero] * 8, axis=0)
        centre, spread = window_stats(series)
        live = place <= lengths_ref[s] - M
        ends_ref[0, s] = jnp.where(live, 2.0, 0.0)
        ends_ref[1, s] = jnp.where(live, 2.0 / (M * spread[:rows]), 0.0)
        for b in range(rows):
            wide = jnp.broadcast_to(centre[b : b + 1], (LANES, LANES))
            centre_ref[s, LANES * b : LANES * (b + 1), :] = wide.T


def spread(block_ref, out_ref, several, left):
    each = several.shape[0]
    for k in range(each):
        several[k] = block_ref[...]
    copies = [
        pltpu.make_async_copy(several, out_ref.at[pl.ds(each * p, each)], left.at[p])
        for p in range(out_ref.shape[0] // each)
    ]
    for copy in copies:
        copy.start()
    for copy in copies:
        copy.wait()


def pick(theirs_ref, gathered_ref, out_ref):
    held, rows, _ = gathered_ref.shape
    slots = theirs_ref.shape[0]
    for s in range(slots):
        want = theirs_ref[s]
        out_ref[rows * s : rows * (s + 1), :] = gathered_ref[want // CORES]
        follow = jnp.minimum((want + 1) // CORES, held - 1)
        out_ref[rows * slots + 8 * s : rows * slots + 8 * (s + 1), :] = gathered_ref[follow, 0:8, :]


def join(overall, core_ref, groups_ref, gathered_ref, passed_ref, windows_ref, centre_ref, ends_ref, out_ref, ref_windows, weights, running, series):
    held, rows, _ = gathered_ref.shape
    slots = groups_ref.shape[0]
    block_len = rows * LANES
    query_len = centre_ref.shape[1]
    tail = rows - M // LANES
    parts = []
    for s in range(slots):
        region = groups_ref[s]
        follow = jnp.minimum((region + 1) // CORES, held - 1)
        block = jnp.where(
            lax.rem(region, CORES) == core_ref[0],
            gathered_ref[region // CORES].astype(jnp.float32),
            passed_ref[rows * s : rows * (s + 1), :].astype(jnp.float32),
        )
        halo = jnp.where(
            lax.rem(region + 1, CORES) == core_ref[0],
            gathered_ref[follow, 0:8, :].astype(jnp.float32),
            passed_ref[rows * slots + 8 * s : rows * slots + 8 * (s + 1), :].astype(jnp.float32),
        )
        parts.append(jnp.concatenate([block, halo], axis=0))
    every = jnp.concatenate(parts, axis=0)
    later = ahead(every, 1)
    centre, spread = window_stats(every)
    inverse = 1.0 / spread
    factors = [inverse, (M * centre) * inverse]
    for s in range(slots):
        first = (rows + 8) * s
        ends = groups_ref[s] * block_len + block_len > overall - M

        def moved(x, x_later, count):
            early = x_later[first + tail - 2 : first + tail - 2 + count]
            return jnp.where(ends, early, x[first + tail : first + tail + count])

        series[s, :rows, :] = every[first : first + rows]
        series[s, rows : rows + 4, :] = moved(every, later, 4)
        for w in range(2):
            weights[w, first : first + tail, :] = factors[w][first : first + tail]
            weights[w, first + tail : first + rows, :] = moved(factors[w], ahead(factors[w], 1), 2)
    lower = lane_iota(LANES) <= lax.broadcasted_iota(jnp.int32, (LANES, LANES), 0)
    own = [None] * slots

    def build(s, b):
        after = sheared(series[s, b : b + 1, :], 1)
        if b not in (0, rows):
            at = lines - LANES * (b - b // rows)
            ref_windows[s, at : at + LANES, :] = jnp.where(lower, own[s], after).astype(jnp.bfloat16)
        own[s] = after

    def finish(s, b):
        best = jnp.max(running[s, LANES * b : LANES * (b + 1), :].T, axis=0, keepdims=True)
        out_ref[s : s + 1, LANES * b : LANES * (b + 1)] = (
            ends_ref[0, s, b : b + 1, :] - best * ends_ref[1, s, b : b + 1, :]
        )

    trips = block_len // (2 * M)
    lines = (rows + 2) * LANES
    pieces = query_len // PIECE

    def compute(*accs):
        def push(u):
            s, t = u // trips, u % trips
            for q in range(2):
                j = lines - M - 2 * M * t - M * q
                if q:
                    j = j - jnp.where(t == trips - 1, LANES, 0)
                tile = [ref_windows[s, pl.ds(pl.multiple_of(j - LANES * h, LANES), M), :] for h in range(2)]
                pltpu.matmul_push_rhs(jnp.concatenate(tile, axis=1), staging_register=0, mxu_index=q)

        def rows_at(u):
            top = (rows + 8) * (u // trips) + 4 * (u % trips)
            return [
                [jnp.broadcast_to(weights[w, pl.ds(top + k, 1), :], (8, LANES)) for k in range(4)] for w in range(2)
            ]

        def drain(u, n, scale, shift):
            s = u // trips
            both = [pltpu.matmul_pop(accs[2 * n + q]) for q in range(2)]
            for r in range(0, PIECE, 8):
                at = PIECE * n + r
                mean = centre_ref[s, at : at + 8, :]
                found = [
                    both[k // 2][r : r + 8, LANES * (k % 2) : LANES * (k % 2 + 1)] * scale[k] - mean * shift[k]
                    for k in range(4)
                ]
                best = jnp.maximum(jnp.maximum(found[0], found[1]), jnp.maximum(found[2], found[3]))
                running[s, at : at + 8, :] = jnp.maximum(running[s, at : at + 8, :], best)

        def trip(u, first, last, extras=()):
            s = u // trips
            extras = list(extras)
            share = -(-len(extras) // pieces)
            before = None if first else rows_at(u - 1)
            now = rows_at(u)
            for n in range(pieces):
                i = PIECE * n
                lhs = jnp.concatenate(
                    [windows_ref[s, i + LANES : i + LANES + PIECE, :], windows_ref[s, i : i + PIECE, :]], axis=1
                )
                if n >= LAG:
                    drain(u, n - LAG, *now)
                elif not first:
                    drain(u - 1, pieces + n - LAG, *before)
                for q in range(2):
                    pltpu.matmul_acc_lhs(accs[2 * n + q], lhs, load_staged_rhs=0 if n == 0 else None)
                for extra in extras[share * n : share * (n + 1)]:
                    extra()
                if n == (pieces - 2 if first else 0) and not last:
                    push(u + 1)
            if last:
                for n in range(pieces - LAG, pieces):
                    drain(u, n, *now)

        for acc in accs:
            pltpu.matmul_pop(acc)
        order = [(s, b) for s in range(slots) for b in range(rows + 4)]
        early = 2 * M // LANES + 2
        for s, b in order[:early]:
            build(s, b)
        push(0)
        trip(0, True, False, [functools.partial(build, s, b) for s, b in order[early:]])

        def middle(u, carry):
            trip(u, False, False)
            return carry

        lax.fori_loop(1, slots * trips - 1, middle, 0)
        done = [(s, b) for s in range(slots - 1) for b in range(query_len // LANES)]
        trip(slots * trips - 1, False, True, [functools.partial(finish, s, b) for s, b in done])
        for b in range(query_len // LANES):
            finish(slots - 1, b)

    running[...] = jnp.full(running.shape, NEVER, jnp.float32)
    pl.run_scoped(
        compute,
        *[pltpu.ACC(n % 2)((PIECE, 2 * LANES), jnp.float32) for n in range(2 * pieces)],
    )


VMEM = pl.BlockSpec(memory_space=pltpu.VMEM)
SMEM = pl.BlockSpec(memory_space=pltpu.SMEM)


def call(kernel, out_shape, in_specs, scratch=(), limit=12 << 20):
    many = isinstance(out_shape, tuple)
    return pl.pallas_call(
        kernel,
        out_shape=out_shape,
        in_specs=in_specs,
        out_specs=(VMEM,) * len(out_shape) if many else VMEM,
        scratch_shapes=scratch,
        compiler_params=pltpu.CompilerParams(vmem_limit_bytes=limit),
    )


def prepare_call(slots, query_len):
    return call(
        prepare_queries,
        (
            jax.ShapeDtypeStruct((slots, query_len + LANES, LANES), jnp.bfloat16),
            jax.ShapeDtypeStruct((slots, query_len, LANES), jnp.float32),
            jax.ShapeDtypeStruct((2, slots, query_len // LANES, LANES), jnp.float32),
        ),
        [SMEM, VMEM, VMEM],
    )


def join_call(slots, rows, query_len, overall):
    return call(
        functools.partial(join, overall),
        jax.ShapeDtypeStruct((slots, query_len), jnp.float32),
        [SMEM, SMEM, VMEM, VMEM, VMEM, VMEM, VMEM],
        [
            pltpu.VMEM((slots, (rows + 2) * LANES, LANES), jnp.bfloat16),
            pltpu.VMEM((2, slots * (rows + 8), LANES), jnp.float32),
            pltpu.VMEM((slots, query_len, LANES), jnp.float32),
            pltpu.VMEM((slots, rows + 8, LANES), jnp.float32),
        ],
    )


def body(long_series, queries, lengths, groups):
    slots, query_len = queries.shape
    rows = long_series.shape[0] // LANES
    chips = lax.axis_size("chip")
    overall = chips * CORES * long_series.shape[0]
    swap = [(0, 1), (1, 0)]
    block = long_series.reshape(rows, LANES)
    copies = pl.pallas_call(
        spread,
        out_shape=jax.ShapeDtypeStruct((chips, rows, LANES), jnp.bfloat16),
        in_specs=[VMEM],
        out_specs=pl.BlockSpec(memory_space=pltpu.HBM),
        scratch_shapes=[pltpu.VMEM((8, rows, LANES), jnp.bfloat16), pltpu.SemaphoreType.DMA((chips // 8,))],
        name="spread",
    )(block)
    gathered = lax.all_to_all(copies, "chip", 0, 0, tiled=True)
    theirs = lax.ppermute(groups, "core", swap)
    windows, centre, ends = prepare_call(slots, query_len)(lengths, queries, queries[:, ::-1])
    picked = call(pick, jax.ShapeDtypeStruct(((rows + 8) * slots, LANES), jnp.bfloat16), [SMEM, VMEM])(theirs, gathered)
    passed = lax.ppermute(picked, "core", swap)
    core = lax.axis_index("core").reshape(1)
    return join_call(slots, rows, query_len, overall)(core, groups, gathered, passed, windows, centre, ends)


def solution(mesh):
    outer, members = mesh.devices.shape
    pairs = Mesh(mesh.devices.reshape(outer, members // CORES, CORES), ("groups", "chip", "core"))
    every = ("groups", "chip", "core")
    return jax.shard_map(
        body,
        mesh=pairs,
        in_specs=(P(every), P(every, None), P(every), P(every)),
        out_specs=P(every, None),
        check_vma=False,
    )
```
